256 devices in a mesh: gx: 4 (over z_lo), gy: 4 (over y), gz: 16 (over x, z_hi, core).
Axes of the slice: x: 4, y: 4, z: 8 (z_hi: 2, z_lo: 4; z = z_hi * 4 + z_lo), core: 2. Of those that a mesh axis runs over, the one named last changes fastest.
Arguments:
- factor_inv: bfloat16 [4, 4096, 16384], P('gx', 'gy', 'gz')
- sep_sizes: int32 [4, 4, 16], P('gx', 'gy', 'gz'), may hold values from 512 to 1024
- coupling: bfloat16 [12, 4096, 16384], P('gx', 'gy', 'gz'), may hold values from -0.109375 to 0.109375
Outputs:
- schur_update: float32 [4, 4096, 16384], P('gx', 'gy', 'gz')
The draws below stay inside these ranges and needn't reach their ends.
All inputs are finite; a program needn't handle non-finite values.
Results may differ from the reference program's by a relative error of at most 0.0023.
Values may be sent and summed in bfloat16 or wider, within the bound.
No kernel may reach another device: no remote copies, remote signals or barrier semaphores. Data moves between devices by JAX's collectives and lax.ppermute only.
A program may use at most 128 MiB of HBM per device.

```python
import jax
import jax.numpy as jnp
from jax import lax

W = 1024
M = 1024
SLOTS = 3
N_GX = 4
N_GY = 4
N_GZ = 16


def draw_factor_inv(key, part):
    first, second = jax.random.split(jax.random.fold_in(key, 11))
    shape = (N_GX, N_GY * W, N_GZ * W)
    rows = lax.broadcasted_iota(jnp.int32, shape, 1) % W
    cols = lax.broadcasted_iota(jnp.int32, shape, 2) % W
    lower = jax.random.normal(first, shape, jnp.float32)
    diag = jax.random.uniform(second, shape, jnp.float32, 0.5, 1.5)
    scaled = lower / jnp.sqrt(jnp.float32(W))
    return jnp.where(rows > cols, scaled, jnp.where(rows == cols, diag, jnp.float32(0.0))).astype(jnp.bfloat16)


def with_ends(entries, key, smallest, high):
    shape = entries.shape
    index_at = [jax.random.randint(jax.random.fold_in(key, axis), (), 0, shape[axis]) for axis in range(len(shape))]
    entries = entries.at[tuple(index_at)].set(smallest)
    longest = shape.index(max(shape))
    index_at[longest] = (index_at[longest] + 1) % shape[longest]
    return entries.at[tuple(index_at)].set(high)


def level_of(own_key, extent, cuts, low, largest):
    def one(dim, blocks):
        steps = jax.random.uniform(jax.random.fold_in(jax.random.fold_in(own_key, 6), dim), (blocks,), jnp.float32, low / len(cuts), largest / len(cuts))
        return jnp.repeat(jnp.exp(steps), extent[dim] // blocks).reshape((-1,) + (1,) * (len(extent) - dim - 1))

    gain = one(*cuts[0])
    for cut in cuts[1:]:
        gain = gain * one(*cut)
    return gain


def gaussian(key, dims, spread, most, cuts=(), held_as=jnp.bfloat16):
    drawn = jax.random.normal(key, dims, jnp.float32) * spread
    if len(cuts) > 0:
        drawn = level_of(key, dims, cuts, -0.22, 0.18) * drawn
    return jnp.clip(drawn, min=-most, max=most).astype(held_as)


def setup_inputs(seed: int = 0) -> dict:
    splits = jax.random.split(jax.random.key(seed), 4)
    factor_inv = draw_factor_inv(jax.random.fold_in(splits[3], 71), 0)
    sep_sizes = with_ends(jax.random.randint(splits[1], (N_GX, N_GY, N_GZ), W // 2, W + 1), jax.random.fold_in(splits[1], 1), W // 2, W).astype(jnp.int32)
    coupling = gaussian(splits[2], (N_GX * SLOTS, N_GY * W, N_GZ * M), (3 * W) ** -0.5, 0.109375, ((0, 4), (1, 4), (2, 16)))
    return dict(factor_inv=factor_inv, sep_sizes=sep_sizes, coupling=coupling)


def reference(factor_inv, sep_sizes, coupling):
    nxa = factor_inv.shape[0]
    nya = factor_inv.shape[1] // W
    nza = factor_inv.shape[2] // W
    inner = jnp.arange(W, dtype=jnp.int32)

    def owned(iidx, jidx, kidx):
        valid = (jidx >= 0) & (jidx < nya) & (kidx >= 0) & (kidx < nza)
        jc = jnp.clip(jidx, 0, nya - 1).astype(jnp.int32)
        kc = jnp.clip(kidx, 0, nza - 1).astype(jnp.int32)
        block = lax.dynamic_slice(factor_inv, (iidx, jc * W, kc * W), (1, W, W))[0]
        count = lax.dynamic_slice(sep_sizes, (iidx, jc, kc), (1, 1, 1))[0, 0, 0]
        keep = ((inner < count) & valid).astype(jnp.bfloat16)
        return block * keep[:, None] * keep[None, :]

    def one(flat):
        iidx = (flat // (nya * nza)).astype(jnp.int32)
        jidx = ((flat // nza) % nya).astype(jnp.int32)
        kidx = (flat % nza).astype(jnp.int32)
        cblock = lax.dynamic_slice(coupling, (iidx * 3, jidx * W, kidx * M), (3, W, M))
        factors = [owned(iidx, jidx, kidx - 1), owned(iidx, jidx, kidx + 1), owned(iidx, jidx - 1, kidx)]
        total = jnp.zeros((M, M), jnp.float32)
        for slot in range(3):
            solved = jnp.dot(factors[slot], cblock[slot], preferred_element_type=jnp.float32).astype(jnp.bfloat16)
            total = total + jnp.dot(solved.T, solved, preferred_element_type=jnp.float32)
        return total

    result = lax.map(one, jnp.arange(nxa * nya * nza, dtype=jnp.int32))
    result = result.reshape(nxa, nya, nza, M, M).transpose(0, 1, 3, 2, 4)
    return result.reshape(nxa, nya * M, nza * M)
```

```python
import functools

import jax
import jax.numpy as jnp
from jax import lax
from jax.experimental import pallas as pl
from jax.experimental.pallas import tpu as pltpu
from jax.sharding import PartitionSpec as P


B = 128
EXTRA = 8
UNITS_FIRST = (0, 1, 2)
UNITS_LAST = (3,)


def pack_kernel(size_ref, f_ref, first_ref, last_ref, full_ref):
    count = size_ref[0, 0, 0]
    n = f_ref.shape[1] // B
    width = n * B
    i = lax.broadcasted_iota(jnp.int32, (B, B), 0)
    j = lax.broadcasted_iota(jnp.int32, (B, B), 1)
    row = lax.broadcasted_iota(jnp.int32, (B, 1), 0)
    diags = []
    for u in range(n // 2):
        big = n - 1 - u
        out, at = (first_ref, EXTRA + B * UNITS_FIRST.index(u)) if u in UNITS_FIRST else (last_ref, B * UNITS_LAST.index(u))
        keep_big = (row + big * B) < count
        keep_small = (row + u * B) < count
        rows_big = f_ref[0, big * B:(big + 1) * B, :]
        rows_big = jnp.where(keep_big, rows_big, jnp.zeros_like(rows_big))
        rows_small = f_ref[0, u * B:(u + 1) * B, :]
        rows_small = jnp.where(keep_small, rows_small, jnp.zeros_like(rows_small))
        d_big = rows_big[:, big * B:(big + 1) * B].astype(jnp.float32)
        d_small = rows_small[:, u * B:(u + 1) * B].astype(jnp.float32)
        square = jnp.where(i >= j, d_small, d_big.T).astype(jnp.bfloat16)
        diags.append(jnp.sum(jnp.where(i == j, d_big, 0.0), axis=0, keepdims=True))
        for ref, to in ((out, at), (full_ref, EXTRA + B * u)):
            ref[to:to + B, 0:big * B] = rows_big[:, 0:big * B]
            ref[to:to + B, big * B:(big + 1) * B] = square
            if u:
                ref[to:to + B, (big + 1) * B:width] = rows_small[:, 0:u * B]
    line = jnp.concatenate(diags + [jnp.zeros((1, width - B * len(diags)), jnp.float32)], axis=1)
    line = jnp.broadcast_to(line, (EXTRA, width)).astype(jnp.bfloat16)
    first_ref[0:EXTRA, :] = line
    full_ref[0:EXTRA, :] = line


def packed(factor_inv, sep_sizes):
    width = factor_inv.shape[1]
    first = EXTRA + B * len(UNITS_FIRST)
    last = B * len(UNITS_LAST)
    return pl.pallas_call(
        pack_kernel,
        out_shape=(
            jax.ShapeDtypeStruct((first, width), jnp.bfloat16),
            jax.ShapeDtypeStruct((last, width), jnp.bfloat16),
            jax.ShapeDtypeStruct((first + last, width), jnp.bfloat16),
        ),
        in_specs=[
            pl.BlockSpec(memory_space=pltpu.SMEM),
            pl.BlockSpec(memory_space=pltpu.VMEM),
        ],
        out_specs=(pl.BlockSpec(memory_space=pltpu.VMEM),) * 3,
        compiler_params=pltpu.CompilerParams(vmem_limit_bytes=12 << 20),
        cost_estimate=pl.CostEstimate(flops=4 * width * width, bytes_accessed=3 * width * width, transcendentals=0),
        name="pack",
    )(sep_sizes, factor_inv)


def place(g, at, unit, u, diag, n):
    i = lax.broadcasted_iota(jnp.int32, (B, B), 0)
    j = lax.broadcasted_iota(jnp.int32, (B, B), 1)
    big = n - 1 - u
    square = unit[:, big * B:(big + 1) * B].astype(jnp.float32)
    lower = jnp.where(i >= j, square, 0.0).astype(jnp.bfloat16)
    line = diag[:, u * B:(u + 1) * B].astype(jnp.float32)
    other = jnp.where(i > j, square.T, jnp.where(i == j, line, 0.0)).astype(jnp.bfloat16)
    lo, hi = at
    if u:
        g[lo:lo + B, 0:u * B] = unit[:, (big + 1) * B:n * B]
    g[lo:lo + B, u * B:(u + 1) * B] = lower
    g[hi:hi + B, 0:big * B] = unit[:, 0:big * B]
    g[hi:hi + B, big * B:(big + 1) * B] = other


def slot_kernel(units, has_acc, which_ref, *refs):
    which = which_ref[0]
    if has_acc:
        acc_ref, *refs = refs
    c_ref, *parts, out_ref, g, x = refs
    first_ref = parts[0]
    n = c_ref.shape[1] // B
    panels = sorted([u for u in units] + [n - 1 - u for u in units])
    where = {p: k * B for k, p in enumerate(panels)}

    @pl.when(pl.program_id(0) == 0)
    def _():
        diag = first_ref[0:1, :]
        g[...] = jnp.zeros_like(g)
        for u in units:
            if len(parts) == 1:
                at = EXTRA + B * u
                unit = first_ref[at:at + B, :]
            else:
                at = B * UNITS_LAST.index(u)
                unit = parts[1][at:at + B, :]
            place(g, (where[u], where[n - 1 - u]), unit, u, diag, n)
        for k in range(0, len(panels), 2):
            depth = (panels[k + 1] + 1) * B
            x[k * B:(k + 2) * B, :] = jnp.dot(
                g[k * B:(k + 2) * B, 0:depth], c_ref[which, 0:depth, :], preferred_element_type=jnp.float32
            ).astype(jnp.bfloat16)

    wide = out_ref.shape[-1]
    cols = pl.ds(pl.multiple_of(pl.program_id(0) * wide, wide), wide)
    part = lax.dot_general(
        x[...], x[:, cols], (((0,), (0,)), ((), ())), preferred_element_type=jnp.float32
    )
    if has_acc:
        part = part + acc_ref[0, :, cols]
    out_ref[0] = part


def update(which, coupling, parts, units, acc):
    width = coupling.shape[1]
    rows = 2 * B * len(units)
    steps = 4
    wide = width // steps
    block = pl.BlockSpec((1, width, wide), lambda s, w: (0, 0, s))
    held = pl.BlockSpec(memory_space=pltpu.VMEM)
    ins = ([acc] if acc is not None else []) + [coupling, *parts]
    specs = [held] * len(ins)
    return pl.pallas_call(
        functools.partial(slot_kernel, units, acc is not None),
        out_shape=jax.ShapeDtypeStruct((1, width, width), jnp.float32),
        grid_spec=pltpu.PrefetchScalarGridSpec(
            num_scalar_prefetch=1,
            grid=(steps,),
            in_specs=specs,
            out_specs=block,
            scratch_shapes=[
                pltpu.VMEM((rows, width), jnp.bfloat16),
                pltpu.VMEM((rows, width), jnp.bfloat16),
            ],
        ),
        cost_estimate=pl.CostEstimate(
            flops=4 * rows * width * width, bytes_accessed=10 * width * width, transcendentals=0
        ),
        compiler_params=pltpu.CompilerParams(vmem_limit_bytes=24 << 20),
    )(which, *ins)


def on_device(factor_inv, sep_sizes, coupling):
    first, last, full = packed(factor_inv, sep_sizes)
    n_z = lax.axis_size("gz")
    n_y = lax.axis_size("gy")
    far_pairs = [p for k in range(1, n_z - 1, 2) for p in ((k, k + 1), (k + 1, k))]
    near_pairs = [p for k in range(0, n_z, 2) for p in ((k, k + 1), (k + 1, k))]
    up = [(k, k + 1) for k in range(n_y - 1)]
    far_first = lax.ppermute(first, "gz", far_pairs)
    far_last = lax.ppermute(last, "gz", far_pairs)
    near = lax.ppermute(full, "gz", near_pairs)
    below_y = lax.ppermute(full, "gy", up)

    odd = lax.axis_index("gz") % 2
    far_slot = jnp.reshape(odd, (1,)).astype(jnp.int32)
    near_slot = 1 - far_slot
    y_slot = jnp.full((1,), 2, jnp.int32)
    every = UNITS_FIRST + UNITS_LAST
    total = update(near_slot, coupling, (near,), every, None)
    total = update(y_slot, coupling, (below_y,), every, total)
    total = update(far_slot, coupling, (far_first,), UNITS_FIRST, total)
    return update(far_slot, coupling, (far_first, far_last), UNITS_LAST, total)


def solution(mesh):
    return jax.shard_map(
        on_device,
        mesh=mesh,
        in_specs=(P("gx", "gy", "gz"), P("gx", "gy", "gz"), P("gx", "gy", "gz")),
        out_specs=P("gx", "gy", "gz"),
        check_vma=False,
    )
```

```python
import functools

import jax
import jax.numpy as jnp
from jax import lax
from jax.experimental import pallas as pl
from jax.experimental.pallas import tpu as pltpu
from jax.sharding import PartitionSpec as P


B = 128
EXTRA = 8
UNITS_FIRST = (0, 1, 2)
UNITS_LAST = (3,)


def pack_kernel(size_ref, f_ref, first_ref, last_ref, full_ref, held, sems):
    count = size_ref[0, 0, 0]
    n = f_ref.shape[1] // B
    width = n * B
    i = lax.broadcasted_iota(jnp.int32, (B, B), 0)
    j = lax.broadcasted_iota(jnp.int32, (B, B), 1)
    row = lax.broadcasted_iota(jnp.int32, (B, 1), 0)

    def copy(p):
        spot = (pl.ds(p * B, B), pl.ds(0, (p + 1) * B))
        return pltpu.make_async_copy(f_ref.at[(0, *spot)], held.at[spot], sems.at[p])

    order = [p for u in range(n // 2) for p in (n - 1 - u, u)]
    for p in order:
        copy(p).start()
    diags = []
    for u in range(n // 2):
        big = n - 1 - u
        out, at = (first_ref, EXTRA + B * UNITS_FIRST.index(u)) if u in UNITS_FIRST else (last_ref, B * UNITS_LAST.index(u))
        copy(big).wait()
        copy(u).wait()
        keep_big = (row + big * B) < count
        keep_small = (row + u * B) < count
        rows_big = held[big * B:(big + 1) * B, 0:(big + 1) * B]
        rows_big = jnp.where(keep_big, rows_big, jnp.zeros_like(rows_big))
        rows_small = held[u * B:(u + 1) * B, 0:(u + 1) * B]
        rows_small = jnp.where(keep_small, rows_small, jnp.zeros_like(rows_small))
        d_big = rows_big[:, big * B:(big + 1) * B].astype(jnp.float32)
        d_small = rows_small[:, u * B:(u + 1) * B].astype(jnp.float32)
        square = jnp.where(i >= j, d_small, d_big.T).astype(jnp.bfloat16)
        diags.append(jnp.sum(jnp.where(i == j, d_big, 0.0), axis=0, keepdims=True))
        for ref, to in ((out, at), (full_ref, EXTRA + B * u)):
            ref[to:to + B, 0:big * B] = rows_big[:, 0:big * B]
            ref[to:to + B, big * B:(big + 1) * B] = square
            if u:
                ref[to:to + B, (big + 1) * B:width] = rows_small[:, 0:u * B]
    line = jnp.concatenate(diags + [jnp.zeros((1, width - B * len(diags)), jnp.float32)], axis=1)
    line = jnp.broadcast_to(line, (EXTRA, width)).astype(jnp.bfloat16)
    first_ref[0:EXTRA, :] = line
    full_ref[0:EXTRA, :] = line


def packed(factor_inv, sep_sizes):
    width = factor_inv.shape[1]
    first = EXTRA + B * len(UNITS_FIRST)
    last = B * len(UNITS_LAST)
    return pl.pallas_call(
        pack_kernel,
        out_shape=tuple(pltpu.VMEM((rows, width), jnp.bfloat16) for rows in (first, last, first + last)),
        in_specs=[
            pl.BlockSpec(memory_space=pltpu.SMEM),
            pl.BlockSpec(memory_space=pltpu.HBM),
        ],
        out_specs=(pl.BlockSpec(memory_space=pltpu.VMEM),) * 3,
        scratch_shapes=[pltpu.VMEM((width, width), jnp.bfloat16), pltpu.SemaphoreType.DMA((width // B,))],
        compiler_params=pltpu.CompilerParams(vmem_limit_bytes=60 << 20),
        cost_estimate=pl.CostEstimate(flops=4 * width * width, bytes_accessed=3 * width * width, transcendentals=0),
        name="pack",
    )(sep_sizes, factor_inv)


def place(g, at, unit, u, diag, n):
    i = lax.broadcasted_iota(jnp.int32, (B, B), 0)
    j = lax.broadcasted_iota(jnp.int32, (B, B), 1)
    big = n - 1 - u
    square = unit[:, big * B:(big + 1) * B].astype(jnp.float32)
    lower = jnp.where(i >= j, square, 0.0).astype(jnp.bfloat16)
    line = diag[:, u * B:(u + 1) * B].astype(jnp.float32)
    other = jnp.where(i > j, square.T, jnp.where(i == j, line, 0.0)).astype(jnp.bfloat16)
    lo, hi = at
    if u:
        g[lo:lo + B, 0:u * B] = unit[:, (big + 1) * B:n * B]
    g[lo:lo + B, u * B:(u + 1) * B] = lower
    g[hi:hi + B, 0:big * B] = unit[:, 0:big * B]
    g[hi:hi + B, big * B:(big + 1) * B] = other


def product(x, depth):
    blocks = x.shape[1] // depth
    for b in range(blocks):
        cols = slice(b * depth, (b + 1) * depth)
        low = slice(b * depth, x.shape[1])
        yield b, cols, low, lax.dot_general(
            x[:, low], x[:, cols], (((0,), (0,)), ((), ())), preferred_element_type=jnp.float32
        )


def slot_kernel(units, has_acc, whole, which_ref, *refs):
    if has_acc:
        acc_ref, *refs = refs
    c_ref, part_ref, out_ref, g, x = refs
    which = which_ref[0]
    n = c_ref.shape[1] // B
    panels = sorted([u for u in units] + [n - 1 - u for u in units])
    where = {p: k * B for k, p in enumerate(panels)}
    for k in range(0, len(panels), 2):
        lo, hi = panels[k], panels[k + 1]
        g[k * B:(k + 1) * B, (lo + 1) * B:(hi + 1) * B] = jnp.zeros((B, (hi - lo) * B), jnp.bfloat16)
    diag = part_ref[0:1, :]
    for u in units:
        at = EXTRA + B * u
        place(g, (where[u], where[n - 1 - u]), part_ref[at:at + B, :], u, diag, n)
    wide = 2 * B
    depths = [(panels[k + 1] + 1) * B for k in range(0, len(panels), 2)]
    for b in range(n // 2):
        cols = slice(b * wide, (b + 1) * wide)
        solved, done, start = None, [], 0
        for k, depth in enumerate(depths):
            part = jnp.dot(
                g[k * wide:, start:depth], c_ref[which, start:depth, cols], preferred_element_type=jnp.float32
            )
            solved = part if solved is None else solved[wide:] + part
            done.append(solved[:wide])
            start = depth
        x[:, cols] = jnp.concatenate(done, axis=0).astype(jnp.bfloat16)
    for b, cols, low, part in product(x, wide):
        if has_acc:
            part = part + acc_ref[0, low, cols]
        out_ref[0, low, cols] = part
        if whole:
            for k in range(b + 1, n // 2):
                out_ref[0, cols, k * wide:(k + 1) * wide] = part[(k - b) * wide:(k - b + 1) * wide].T


def update(which, coupling, part, units, acc, whole=False):
    width = coupling.shape[1]
    rows = 2 * B * len(units)
    ins = ([acc] if acc is not None else []) + [coupling, part]
    return pl.pallas_call(
        functools.partial(slot_kernel, units, acc is not None, whole),
        out_shape=jax.ShapeDtypeStruct((1, width, width), jnp.float32),
        in_specs=[pl.BlockSpec(memory_space=pltpu.SMEM)] + [pl.BlockSpec(memory_space=pltpu.VMEM)] * len(ins),
        out_specs=pl.BlockSpec(memory_space=pltpu.VMEM),
        scratch_shapes=[
            pltpu.VMEM((rows, width), jnp.bfloat16),
            pltpu.VMEM((rows, width), jnp.bfloat16),
        ],
        compiler_params=pltpu.CompilerParams(vmem_limit_bytes=24 << 20),
        cost_estimate=pl.CostEstimate(
            flops=4 * rows * width * width, bytes_accessed=10 * width * width, transcendentals=0
        ),
    )(which, *ins)


def last_kernel(which_ref, acc_ref, c_ref, first_ref, *refs):
    last_refs, (out_ref, g, x, sums, sems) = refs[:-5], refs[-5:]
    which = which_ref[0]
    n = c_ref.shape[1] // B
    panels = sorted([u for u in UNITS_LAST] + [n - 1 - u for u in UNITS_LAST])
    where = {p: k * B for k, p in enumerate(panels)}
    for k in range(0, len(panels), 2):
        lo, hi = panels[k], panels[k + 1]
        g[k * B:(k + 1) * B, (lo + 1) * B:(hi + 1) * B] = jnp.zeros((B, (hi - lo) * B), jnp.bfloat16)
    for u in UNITS_LAST:
        at = B * UNITS_LAST.index(u)
        unit = sum((ref[at:at + B, :] for ref in last_refs[1:]), last_refs[0][at:at + B, :])
        place(g, (where[u], where[n - 1 - u]), unit, u, first_ref[0:1, :], n)
    blocks = 4
    wide = n * B // blocks
    cut = [slice(b * wide, (b + 1) * wide) for b in range(blocks)]
    for cols in cut:
        for k in range(0, len(panels), 2):
            depth = (panels[k + 1] + 1) * B
            x[k * B:(k + 2) * B, cols] = jnp.dot(
                g[k * B:(k + 2) * B, 0:depth], c_ref[which, 0:depth, cols], preferred_element_type=jnp.float32
            ).astype(jnp.bfloat16)

    def copy(b):
        cols = pl.ds(b * wide, wide)
        return pltpu.make_async_copy(sums.at[:, cols], out_ref.at[0, :, cols], sems.at[b])

    for b, cols in enumerate(cut):
        part = lax.dot_general(x[...], x[:, cols], (((0,), (0,)), ((), ())), preferred_element_type=jnp.float32)
        sums[:, cols] = acc_ref[0, :, cols] + part
        copy(b).start()
    for b in range(blocks):
        copy(b).wait()


def last_update(which, coupling, parts, acc):
    width = coupling.shape[1]
    rows = 2 * B * len(UNITS_LAST)
    return pl.pallas_call(
        last_kernel,
        out_shape=jax.ShapeDtypeStruct((1, width, width), jnp.float32),
        in_specs=[pl.BlockSpec(memory_space=pltpu.SMEM)] + [pl.BlockSpec(memory_space=pltpu.VMEM)] * (2 + len(parts)),
        out_specs=pl.BlockSpec(memory_space=pltpu.HBM),
        scratch_shapes=[
            pltpu.VMEM((rows, width), jnp.bfloat16),
            pltpu.VMEM((rows, width), jnp.bfloat16),
            pltpu.VMEM((width, width), jnp.float32),
            pltpu.SemaphoreType.DMA((4,)),
        ],
        compiler_params=pltpu.CompilerParams(vmem_limit_bytes=16 << 20),
        cost_estimate=pl.CostEstimate(
            flops=4 * rows * width * width, bytes_accessed=10 * width * width, transcendentals=0
        ),
        name="last",
    )(which, acc, coupling, *parts)


def moved(block, pairs):
    return lax.ppermute(block, ("gx", "gy", "gz"), pairs)


def routes(n_lo, n_y, n_z):
    big, small, near, up = [], [], [], []
    aside, beside, rising, falling = (([], []) for _ in range(4))
    columns = n_z // 4
    for lo in range(n_lo):
        for y in range(n_y):
            at = lambda k: (lo * n_y + y) * n_z + k
            for k in range(0, n_z, 2):
                near += [(at(k), at(k + 1)), (at(k + 1), at(k))]
            if y + 1 < n_y:
                up += [(at(k), at(k) + n_z) for k in range(n_z)]
            for x in range(columns):
                for pair in ((4 * x + 1, 4 * x + 2), (4 * x + 2, 4 * x + 1)):
                    big.append(tuple(map(at, pair)))
                    small.append(tuple(map(at, pair)))
            end = 4 * (columns - 1)
            for x in range(columns - 1):
                right, left = 4 * x + 3, 4 * x + 4
                turn, side = divmod(columns - 2 - x, 2)
                back, other = divmod(x, 2)
                for source, target, relay, first, onward, which in (
                    (right, left, end + 3 - side, aside, rising, turn),
                    (left, right, other, beside, falling, back),
                ):
                    big.append((at(source), at(target)))
                    first[which].append((at(source), at(relay)))
                    onward[which].append((at(relay), at(target)))
    return big, small, aside, rising, beside, falling, near, up


def on_device(factor_inv, sep_sizes, coupling):
    first, last, full = packed(factor_inv, sep_sizes)
    big, small, aside, rising, beside, falling, near_pairs, up = routes(*(lax.axis_size(a) for a in ("gx", "gy", "gz")))
    far_first = moved(first, big)
    side_a = moved(last, aside[0])
    side_b = moved(last, aside[1])
    far_last = moved(last, small)
    rising_a = moved(side_a, rising[0])
    rising_b = moved(side_b, rising[1])
    below_y = moved(full, up)
    side_c = moved(last, beside[0])
    side_d = moved(last, beside[1])
    falling_a = moved(side_c, falling[0])
    falling_b = moved(side_d, falling[1])
    near = moved(full, near_pairs)

    odd = lax.axis_index("gz") % 2
    far_slot = jnp.reshape(odd, (1,)).astype(jnp.int32)
    near_slot = 1 - far_slot
    y_slot = jnp.full((1,), 2, jnp.int32)
    every = UNITS_FIRST + UNITS_LAST
    total = update(near_slot, coupling, near, every, None)
    total = update(y_slot, coupling, below_y, every, total)
    total = update(far_slot, coupling, far_first, UNITS_FIRST, total, whole=True)
    return last_update(far_slot, coupling, (far_first, far_last, rising_a, rising_b, falling_a, falling_b), total)


def solution(mesh):
    return jax.shard_map(
        on_device,
        mesh=mesh,
        in_specs=(P("gx", "gy", "gz"), P("gx", "gy", "gz"), P("gx", "gy", "gz")),
        out_specs=P("gx", "gy", "gz"),
        check_vma=False,
    )
```

```python
import functools

import jax
import jax.numpy as jnp
from jax import lax
from jax.experimental import pallas as pl
from jax.experimental.pallas import tpu as pltpu
from jax.sharding import PartitionSpec as P


B = 128
EXTRA = 8
UNITS_FIRST = (0, 1, 2)
UNITS_LAST = (3,)


def pack_kernel(size_ref, f_ref, first_ref, last_ref, full_ref, held, sems):
    count = size_ref[0, 0, 0]
    n = f_ref.shape[1] // B
    width = n * B
    i = lax.broadcasted_iota(jnp.int32, (B, B), 0)
    j = lax.broadcasted_iota(jnp.int32, (B, B), 1)
    row = lax.broadcasted_iota(jnp.int32, (B, 1), 0)

    def copy(p):
        spot = (pl.ds(p * B, B), pl.ds(0, (p + 1) * B))
        return pltpu.make_async_copy(f_ref.at[(0, *spot)], held.at[spot], sems.at[p])

    order = [p for u in range(n // 2) for p in (n - 1 - u, u)]
    for p in order:
        copy(p).start()
    diags = []
    for u in range(n // 2):
        big = n - 1 - u
        out, at = (first_ref, EXTRA + B * UNITS_FIRST.index(u)) if u in UNITS_FIRST else (last_ref, B * UNITS_LAST.index(u))
        copy(big).wait()
        copy(u).wait()
        keep_big = (row + big * B) < count
        keep_small = (row + u * B) < count
        rows_big = held[big * B:(big + 1) * B, 0:(big + 1) * B]
        rows_big = jnp.where(keep_big, rows_big, jnp.zeros_like(rows_big))
        rows_small = held[u * B:(u + 1) * B, 0:(u + 1) * B]
        rows_small = jnp.where(keep_small, rows_small, jnp.zeros_like(rows_small))
        d_big = rows_big[:, big * B:(big + 1) * B].astype(jnp.float32)
        d_small = rows_small[:, u * B:(u + 1) * B].astype(jnp.float32)
        square = jnp.where(i >= j, d_small, d_big.T).astype(jnp.bfloat16)
        diags.append(jnp.sum(jnp.where(i == j, d_big, 0.0), axis=0, keepdims=True))
        for ref, to in ((out, at), (full_ref, EXTRA + B * u)):
            ref[to:to + B, 0:big * B] = rows_big[:, 0:big * B]
            ref[to:to + B, big * B:(big + 1) * B] = square
            if u:
                ref[to:to + B, (big + 1) * B:width] = rows_small[:, 0:u * B]
    line = jnp.concatenate(diags + [jnp.zeros((1, width - B * len(diags)), jnp.float32)], axis=1)
    line = jnp.broadcast_to(line, (EXTRA, width)).astype(jnp.bfloat16)
    first_ref[0:EXTRA, :] = line
    full_ref[0:EXTRA, :] = line


def packed(factor_inv, sep_sizes):
    width = factor_inv.shape[1]
    first = EXTRA + B * len(UNITS_FIRST)
    last = B * len(UNITS_LAST)
    return pl.pallas_call(
        pack_kernel,
        out_shape=tuple(pltpu.VMEM((rows, width), jnp.bfloat16) for rows in (first, last, first + last)),
        in_specs=[
            pl.BlockSpec(memory_space=pltpu.SMEM),
            pl.BlockSpec(memory_space=pltpu.HBM),
        ],
        out_specs=(pl.BlockSpec(memory_space=pltpu.VMEM),) * 3,
        scratch_shapes=[pltpu.VMEM((width, width), jnp.bfloat16), pltpu.SemaphoreType.DMA((width // B,))],
        compiler_params=pltpu.CompilerParams(vmem_limit_bytes=57 << 20),
        cost_estimate=pl.CostEstimate(flops=4 * width * width, bytes_accessed=3 * width * width, transcendentals=0),
        name="pack",
    )(sep_sizes, factor_inv)


def place(g, at, unit, u, diag, n):
    i = lax.broadcasted_iota(jnp.int32, (B, B), 0)
    j = lax.broadcasted_iota(jnp.int32, (B, B), 1)
    big = n - 1 - u
    square = unit[:, big * B:(big + 1) * B].astype(jnp.float32)
    lower = jnp.where(i >= j, square, 0.0).astype(jnp.bfloat16)
    line = diag[:, u * B:(u + 1) * B].astype(jnp.float32)
    other = jnp.where(i > j, square.T, jnp.where(i == j, line, 0.0)).astype(jnp.bfloat16)
    lo, hi = at
    if u:
        g[lo:lo + B, 0:u * B] = unit[:, (big + 1) * B:n * B]
    g[lo:lo + B, u * B:(u + 1) * B] = lower
    g[hi:hi + B, 0:big * B] = unit[:, 0:big * B]
    g[hi:hi + B, big * B:(big + 1) * B] = other


def product(x, depth):
    blocks = x.shape[1] // depth
    for b in range(blocks):
        cols = slice(b * depth, (b + 1) * depth)
        low = slice(b * depth, x.shape[1])
        yield b, cols, low, lax.dot_general(
            x[:, low], x[:, cols], (((0,), (0,)), ((), ())), preferred_element_type=jnp.float32
        )


def gathered(refs, rows):
    return sum((ref[rows, :] for ref in refs[1:]), refs[0][rows, :])


def slot_kernel(units, has_acc, whole, which_ref, *refs):
    if has_acc:
        acc_ref, *refs = refs
    c_ref, *part_refs, out_ref, g, x = refs
    which = which_ref[0]
    n = c_ref.shape[1] // B
    panels = sorted([u for u in units] + [n - 1 - u for u in units])
    where = {p: k * B for k, p in enumerate(panels)}
    for k in range(0, len(panels), 2):
        lo, hi = panels[k], panels[k + 1]
        g[k * B:(k + 1) * B, (lo + 1) * B:(hi + 1) * B] = jnp.zeros((B, (hi - lo) * B), jnp.bfloat16)
    diag = gathered(part_refs, slice(0, 1))
    for u in units:
        at = EXTRA + B * u
        place(g, (where[u], where[n - 1 - u]), gathered(part_refs, slice(at, at + B)), u, diag, n)
    wide = 2 * B
    depths = [(panels[k + 1] + 1) * B for k in range(0, len(panels), 2)]
    for b in range(n // 2):
        cols = slice(b * wide, (b + 1) * wide)
        solved, done, start = None, [], 0
        for k, depth in enumerate(depths):
            part = jnp.dot(
                g[k * wide:, start:depth], c_ref[which, start:depth, cols], preferred_element_type=jnp.float32
            )
            solved = part if solved is None else solved[wide:] + part
            done.append(solved[:wide])
            start = depth
        x[:, cols] = jnp.concatenate(done, axis=0).astype(jnp.bfloat16)
    for b, cols, low, part in product(x, wide):
        if has_acc:
            part = part + acc_ref[0, low, cols]
        out_ref[0, low, cols] = part
        if whole:
            for k in range(b + 1, n // 2):
                out_ref[0, cols, k * wide:(k + 1) * wide] = part[(k - b) * wide:(k - b + 1) * wide].T


def update(which, coupling, parts, units, acc, whole=False):
    width = coupling.shape[1]
    rows = 2 * B * len(units)
    ins = ([acc] if acc is not None else []) + [coupling, *parts]
    return pl.pallas_call(
        functools.partial(slot_kernel, units, acc is not None, whole),
        out_shape=jax.ShapeDtypeStruct((1, width, width), jnp.float32),
        in_specs=[pl.BlockSpec(memory_space=pltpu.SMEM)] + [pl.BlockSpec(memory_space=pltpu.VMEM)] * len(ins),
        out_specs=pl.BlockSpec(memory_space=pltpu.VMEM),
        scratch_shapes=[
            pltpu.VMEM((rows, width), jnp.bfloat16),
            pltpu.VMEM((rows, width), jnp.bfloat16),
        ],
        compiler_params=pltpu.CompilerParams(vmem_limit_bytes=12 << 20),
        cost_estimate=pl.CostEstimate(
            flops=4 * rows * width * width, bytes_accessed=10 * width * width, transcendentals=0
        ),
    )(which, *ins)


def last_kernel(which_ref, acc_ref, c_ref, first_ref, *refs):
    last_refs, (out_ref, g, x, sums, sems) = refs[:3], refs[-5:]
    which = which_ref[0]
    n = c_ref.shape[1] // B
    panels = sorted([u for u in UNITS_LAST] + [n - 1 - u for u in UNITS_LAST])
    where = {p: k * B for k, p in enumerate(panels)}
    for k in range(0, len(panels), 2):
        lo, hi = panels[k], panels[k + 1]
        g[k * B:(k + 1) * B, (lo + 1) * B:(hi + 1) * B] = jnp.zeros((B, (hi - lo) * B), jnp.bfloat16)
    for u in UNITS_LAST:
        at = B * UNITS_LAST.index(u)
        unit = gathered(last_refs, slice(at, at + B))
        place(g, (where[u], where[n - 1 - u]), unit, u, first_ref[0:1, :], n)
    blocks = 4
    wide = n * B // blocks
    cut = [slice(b * wide, (b + 1) * wide) for b in range(blocks)]
    for cols in cut:
        for k in range(0, len(panels), 2):
            depth = (panels[k + 1] + 1) * B
            x[k * B:(k + 2) * B, cols] = jnp.dot(
                g[k * B:(k + 2) * B, 0:depth], c_ref[which, 0:depth, cols], preferred_element_type=jnp.float32
            ).astype(jnp.bfloat16)

    def copy(b):
        cols = pl.ds(b * wide, wide)
        return pltpu.make_async_copy(sums.at[:, cols], out_ref.at[0, :, cols], sems.at[b])

    for b, cols in enumerate(cut):
        part = lax.dot_general(x[...], x[:, cols], (((0,), (0,)), ((), ())), preferred_element_type=jnp.float32)
        sums[:, cols] = acc_ref[0, :, cols] + part
        copy(b).start()
    for b in range(blocks):
        copy(b).wait()


def last_update(which, coupling, parts, acc):
    width = coupling.shape[1]
    rows = 2 * B * len(UNITS_LAST)
    return pl.pallas_call(
        last_kernel,
        out_shape=jax.ShapeDtypeStruct((1, width, width), jnp.float32),
        in_specs=[pl.BlockSpec(memory_space=pltpu.SMEM)] + [pl.BlockSpec(memory_space=pltpu.VMEM)] * (2 + len(parts)),
        out_specs=pl.BlockSpec(memory_space=pltpu.HBM),
        scratch_shapes=[
            pltpu.VMEM((rows, width), jnp.bfloat16),
            pltpu.VMEM((rows, width), jnp.bfloat16),
            pltpu.VMEM((width, width), jnp.float32),
            pltpu.SemaphoreType.DMA((4,)),
        ],
        compiler_params=pltpu.CompilerParams(vmem_limit_bytes=10 << 20),
        cost_estimate=pl.CostEstimate(
            flops=4 * rows * width * width, bytes_accessed=10 * width * width, transcendentals=0
        ),
        name="last",
    )(which, acc, coupling, *parts)


def moved(block, pairs):
    return lax.ppermute(block, ("gx", "gy", "gz"), pairs)


def routes(n_lo, n_y, n_z):
    big, small, near, up, late = [], [], [], [], []
    aside, onward = ([], []), ([], [])
    columns = n_z // 4
    for lo in range(n_lo):
        for y in range(n_y):
            at = lambda k: (lo * n_y + y) * n_z + k
            for k in range(0, n_z, 2):
                near += [(at(k), at(k + 1)), (at(k + 1), at(k))]
            if y + 1 < n_y:
                for k in range(n_z):
                    relays = k % 2 == 0 if k % 4 < 2 else k == n_z - 1
                    (late if relays else up).append((at(k), at(k) + n_z))
            for x in range(columns):
                for pair in ((4 * x + 1, 4 * x + 2), (4 * x + 2, 4 * x + 1)):
                    big.append(tuple(map(at, pair)))
                    small.append(tuple(map(at, pair)))
            end = 4 * (columns - 1)
            for x in range(columns - 1):
                right, left = 4 * x + 3, 4 * x + 4
                turn, side = divmod(columns - 2 - x, 2)
                back, other = divmod(x, 2)
                for source, target, relay, which in (
                    (right, left, end + 3 - side, turn),
                    (left, right, other, back),
                ):
                    big.append((at(source), at(target)))
                    aside[which].append((at(source), at(relay)))
                    onward[which].append((at(relay), at(target)))
    return big, small, aside, onward, near, up, late


def on_device(factor_inv, sep_sizes, coupling):
    first, last, full = packed(factor_inv, sep_sizes)
    big, small, aside, onward, near_pairs, up, late = routes(*(lax.axis_size(a) for a in ("gx", "gy", "gz")))
    far_first = moved(first, big)
    side_a = moved(last, aside[0])
    side_b = moved(last, aside[1])
    far_last = moved(last, small)
    below_y = moved(full, up)
    on_a = moved(side_a, onward[0])
    on_b = moved(side_b, onward[1])
    late_y = moved(full, late)
    near = moved(full, near_pairs)

    odd = lax.axis_index("gz") % 2
    far_slot = jnp.reshape(odd, (1,)).astype(jnp.int32)
    near_slot = 1 - far_slot
    y_slot = jnp.full((1,), 2, jnp.int32)
    every = UNITS_FIRST + UNITS_LAST
    total = update(near_slot, coupling, (near,), every, None)
    total = update(y_slot, coupling, (below_y, late_y), every, total)
    total = update(far_slot, coupling, (far_first,), UNITS_FIRST, total, whole=True)
    return last_update(far_slot, coupling, (far_first, *(far_last, on_a, on_b) * 4), total)


def solution(mesh):
    return jax.shard_map(
        on_device,
        mesh=mesh,
        in_specs=(P("gx", "gy", "gz"), P("gx", "gy", "gz"), P("gx", "gy", "gz")),
        out_specs=P("gx", "gy", "gz"),
        check_vma=False,
    )
```

```python
import functools

import jax
import jax.numpy as jnp
from jax import lax
from jax.experimental import pallas as pl
from jax.experimental.pallas import tpu as pltpu
from jax.sharding import PartitionSpec as P


B = 128
EXTRA = 8
UNITS_FIRST = (0, 1, 2)
UNITS_LAST = (3,)


def pack_kernel(size_ref, f_ref, first_ref, last_ref, full_ref, held, sems):
    count = size_ref[0, 0, 0]
    n = f_ref.shape[1] // B
    i = lax.broadcasted_iota(jnp.int32, (B, B), 0)
    j = lax.broadcasted_iota(jnp.int32, (B, B), 1)
    row = lax.broadcasted_iota(jnp.int32, (B, 1), 0)

    def copy(p):
        spot = (pl.ds(p * B, B), pl.ds(0, (p + 1) * B))
        return pltpu.make_async_copy(f_ref.at[(0, *spot)], held.at[spot], sems.at[p])

    order = [p for u in range(n // 2) for p in (n - 1 - u, u)]
    for p in order:
        copy(p).start()
    diags = []
    for u in range(n // 2):
        big = n - 1 - u
        out, at = (first_ref, UNITS_FIRST.index(u)) if u in UNITS_FIRST else (last_ref, UNITS_LAST.index(u))
        copy(big).wait()
        copy(u).wait()
        keep_big = (row + big * B) < count
        keep_small = (row + u * B) < count
        rows_big = held[big * B:(big + 1) * B, 0:(big + 1) * B]
        rows_big = jnp.where(keep_big, rows_big, jnp.zeros_like(rows_big))
        rows_small = held[u * B:(u + 1) * B, 0:(u + 1) * B]
        rows_small = jnp.where(keep_small, rows_small, jnp.zeros_like(rows_small))
        d_big = rows_big[:, big * B:(big + 1) * B].astype(jnp.float32)
        d_small = rows_small[:, u * B:(u + 1) * B].astype(jnp.float32)
        square = jnp.where(i >= j, d_small, d_big.T).astype(jnp.bfloat16)
        diags.append(jnp.sum(jnp.where(i == j, d_big, 0.0), axis=0, keepdims=True))
        blocks = [rows_big[:, c * B:(c + 1) * B] for c in range(big)] + [square]
        blocks += [rows_small[:, c * B:(c + 1) * B] for c in range(u)]
        for ref, to in ((out, at * n), (full_ref, u * n)):
            for c, block in enumerate(blocks):
                ref[(to + c) * B:(to + c + 1) * B, :] = block
    lines = jnp.concatenate(diags + [jnp.zeros((EXTRA - len(diags), B), jnp.float32)], axis=0)
    lines = lines.astype(jnp.bfloat16)
    first_ref[first_ref.shape[0] - EXTRA:, :] = lines
    full_ref[full_ref.shape[0] - EXTRA:, :] = lines


def packed(factor_inv, sep_sizes):
    width = factor_inv.shape[1]
    first = EXTRA + width * len(UNITS_FIRST)
    last = width * len(UNITS_LAST)
    return pl.pallas_call(
        pack_kernel,
        out_shape=tuple(jax.ShapeDtypeStruct((rows, B), jnp.bfloat16) for rows in (first, last, first + last)),
        in_specs=[
            pl.BlockSpec(memory_space=pltpu.SMEM),
            pl.BlockSpec(memory_space=pltpu.HBM),
        ],
        out_specs=(pl.BlockSpec(memory_space=pltpu.VMEM),) * 3,
        scratch_shapes=[pltpu.VMEM((width, width), jnp.bfloat16), pltpu.SemaphoreType.DMA((width // B,))],
        compiler_params=pltpu.CompilerParams(vmem_limit_bytes=51 << 20),
        cost_estimate=pl.CostEstimate(flops=4 * width * width, bytes_accessed=3 * width * width, transcendentals=0),
        name="pack",
    )(sep_sizes, factor_inv)


def place(g, at, unit, u, diag, n):
    i = lax.broadcasted_iota(jnp.int32, (B, B), 0)
    j = lax.broadcasted_iota(jnp.int32, (B, B), 1)
    big = n - 1 - u
    square = unit[big * B:(big + 1) * B, :].astype(jnp.float32)
    lower = jnp.where(i >= j, square, 0.0).astype(jnp.bfloat16)
    line = diag[u:u + 1, :].astype(jnp.float32)
    other = jnp.where(i > j, square.T, jnp.where(i == j, line, 0.0)).astype(jnp.bfloat16)
    lo, hi = at
    for c in range(u):
        g[lo:lo + B, c * B:(c + 1) * B] = unit[(big + 1 + c) * B:(big + 2 + c) * B, :]
    g[lo:lo + B, u * B:(u + 1) * B] = lower
    for c in range(big):
        g[hi:hi + B, c * B:(c + 1) * B] = unit[c * B:(c + 1) * B, :]
    g[hi:hi + B, big * B:(big + 1) * B] = other


def product(x, depth):
    blocks = x.shape[1] // depth
    for b in range(blocks):
        cols = slice(b * depth, (b + 1) * depth)
        low = slice(b * depth, x.shape[1])
        yield b, cols, low, lax.dot_general(
            x[:, low], x[:, cols], (((0,), (0,)), ((), ())), preferred_element_type=jnp.float32
        )


def gathered(refs, rows):
    return sum((ref[rows, :] for ref in refs[1:]), refs[0][rows, :])


def slot_kernel(units, has_acc, whole, which_ref, *refs):
    if has_acc:
        acc_ref, *refs = refs
    c_ref, *part_refs, out_ref, g, x = refs
    which = which_ref[0]
    n = c_ref.shape[1] // B
    panels = sorted([u for u in units] + [n - 1 - u for u in units])
    where = {p: k * B for k, p in enumerate(panels)}
    for k in range(0, len(panels), 2):
        lo, hi = panels[k], panels[k + 1]
        g[k * B:(k + 1) * B, (lo + 1) * B:(hi + 1) * B] = jnp.zeros((B, (hi - lo) * B), jnp.bfloat16)
    lines = len(units) * n * B
    diag = gathered(part_refs, slice(lines, lines + EXTRA))
    for u in units:
        at = u * n * B
        place(g, (where[u], where[n - 1 - u]), gathered(part_refs, slice(at, at + n * B)), u, diag, n)
    wide = 2 * B
    depths = [(panels[k + 1] + 1) * B for k in range(0, len(panels), 2)]
    for b in range(n // 2):
        cols = slice(b * wide, (b + 1) * wide)
        solved, done, start = None, [], 0
        for k, depth in enumerate(depths):
            part = jnp.dot(
                g[k * wide:, start:depth], c_ref[which, start:depth, cols], preferred_element_type=jnp.float32
            )
            solved = part if solved is None else solved[wide:] + part
            done.append(solved[:wide])
            start = depth
        x[:, cols] = jnp.concatenate(done, axis=0).astype(jnp.bfloat16)
    for b, cols, low, part in product(x, wide):
        if has_acc:
            part = part + acc_ref[0, low, cols]
        out_ref[0, low, cols] = part
        if whole:
            for k in range(b + 1, n // 2):
                out_ref[0, cols, k * wide:(k + 1) * wide] = part[(k - b) * wide:(k - b + 1) * wide].T


def update(which, coupling, parts, units, acc, whole=False):
    width = coupling.shape[1]
    rows = 2 * B * len(units)
    ins = ([acc] if acc is not None else []) + [coupling, *parts]
    return pl.pallas_call(
        functools.partial(slot_kernel, units, acc is not None, whole),
        out_shape=jax.ShapeDtypeStruct((1, width, width), jnp.float32),
        in_specs=[pl.BlockSpec(memory_space=pltpu.SMEM)] + [pl.BlockSpec(memory_space=pltpu.VMEM)] * len(ins),
        out_specs=pl.BlockSpec(memory_space=pltpu.VMEM),
        scratch_shapes=[
            pltpu.VMEM((rows, width), jnp.bfloat16),
            pltpu.VMEM((rows, width), jnp.bfloat16),
        ],
        compiler_params=pltpu.CompilerParams(vmem_limit_bytes=12 << 20),
        cost_estimate=pl.CostEstimate(
            flops=4 * rows * width * width, bytes_accessed=10 * width * width, transcendentals=0
        ),
    )(which, *ins)


def last_kernel(which_ref, acc_ref, c_ref, first_ref, *refs):
    last_refs, (out_ref, g, x, sums, sems) = refs[:3], refs[-5:]
    which = which_ref[0]
    n = c_ref.shape[1] // B
    panels = sorted([u for u in UNITS_LAST] + [n - 1 - u for u in UNITS_LAST])
    where = {p: k * B for k, p in enumerate(panels)}
    for k in range(0, len(panels), 2):
        lo, hi = panels[k], panels[k + 1]
        g[k * B:(k + 1) * B, (lo + 1) * B:(hi + 1) * B] = jnp.zeros((B, (hi - lo) * B), jnp.bfloat16)
    for u in UNITS_LAST:
        at = n * B * UNITS_LAST.index(u)
        unit = gathered(last_refs, slice(at, at + n * B))
        place(g, (where[u], where[n - 1 - u]), unit, u, first_ref[first_ref.shape[0] - EXTRA:, :], n)
    blocks = 4
    wide = n * B // blocks
    cut = [slice(b * wide, (b + 1) * wide) for b in range(blocks)]
    for cols in cut:
        for k in range(0, len(panels), 2):
            depth = (panels[k + 1] + 1) * B
            x[k * B:(k + 2) * B, cols] = jnp.dot(
                g[k * B:(k + 2) * B, 0:depth], c_ref[which, 0:depth, cols], preferred_element_type=jnp.float32
            ).astype(jnp.bfloat16)

    def copy(b):
        cols = pl.ds(b * wide, wide)
        return pltpu.make_async_copy(sums.at[:, cols], out_ref.at[0, :, cols], sems.at[b])

    for b, cols in enumerate(cut):
        part = lax.dot_general(x[...], x[:, cols], (((0,), (0,)), ((), ())), preferred_element_type=jnp.float32)
        sums[:, cols] = acc_ref[0, :, cols] + part
        copy(b).start()
    for b in range(blocks):
        copy(b).wait()


def last_update(which, coupling, parts, acc):
    width = coupling.shape[1]
    rows = 2 * B * len(UNITS_LAST)
    return pl.pallas_call(
        last_kernel,
        out_shape=jax.ShapeDtypeStruct((1, width, width), jnp.float32),
        in_specs=[pl.BlockSpec(memory_space=pltpu.SMEM)] + [pl.BlockSpec(memory_space=pltpu.VMEM)] * (2 + len(parts)),
        out_specs=pl.BlockSpec(memory_space=pltpu.HBM),
        scratch_shapes=[
            pltpu.VMEM((rows, width), jnp.bfloat16),
            pltpu.VMEM((rows, width), jnp.bfloat16),
            pltpu.VMEM((width, width), jnp.float32),
            pltpu.SemaphoreType.DMA((4,)),
        ],
        compiler_params=pltpu.CompilerParams(vmem_limit_bytes=10 << 20),
        cost_estimate=pl.CostEstimate(
            flops=4 * rows * width * width, bytes_accessed=10 * width * width, transcendentals=0
        ),
        name="last",
    )(which, acc, coupling, *parts)


def moved(block, pairs):
    return lax.ppermute(block, ("gx", "gy", "gz"), pairs)


def routes(n_lo, n_y, n_z):
    big, small, near, up, late = [], [], [], [], []
    aside, onward = ([], []), ([], [])
    columns = n_z // 4
    for lo in range(n_lo):
        for y in range(n_y):
            at = lambda k: (lo * n_y + y) * n_z + k
            for k in range(0, n_z, 2):
                near += [(at(k), at(k + 1)), (at(k + 1), at(k))]
            if y + 1 < n_y:
                for k in range(n_z):
                    relays = k % 2 == 0 if k % 4 < 2 else k == n_z - 1
                    (late if relays else up).append((at(k), at(k) + n_z))
            for x in range(columns):
                for pair in ((4 * x + 1, 4 * x + 2), (4 * x + 2, 4 * x + 1)):
                    big.append(tuple(map(at, pair)))
                    small.append(tuple(map(at, pair)))
            end = 4 * (columns - 1)
            for x in range(columns - 1):
                right, left = 4 * x + 3, 4 * x + 4
                turn, side = divmod(columns - 2 - x, 2)
                back, other = divmod(x, 2)
                for source, target, relay, which in (
                    (right, left, end + 3 - side, turn),
                    (left, right, other, back),
                ):
                    big.append((at(source), at(target)))
                    aside[which].append((at(source), at(relay)))
                    onward[which].append((at(relay), at(target)))
    return big, small, aside, onward, near, up, late


def on_device(factor_inv, sep_sizes, coupling):
    first, last, full = packed(factor_inv, sep_sizes)
    big, small, aside, onward, near_pairs, up, late = routes(*(lax.axis_size(a) for a in ("gx", "gy", "gz")))
    far_first = moved(first, big)
    side_a = moved(last, aside[0])
    side_b = moved(last, aside[1])
    far_last = moved(last, small)
    below_y = moved(full, up)
    on_a = moved(side_a, onward[0])
    on_b = moved(side_b, onward[1])
    late_y = moved(full, late)
    near = moved(full, near_pairs)

    odd = lax.axis_index("gz") % 2
    far_slot = jnp.reshape(odd, (1,)).astype(jnp.int32)
    near_slot = 1 - far_slot
    y_slot = jnp.full((1,), 2, jnp.int32)
    every = UNITS_FIRST + UNITS_LAST
    total = update(near_slot, coupling, (near,), every, None)
    total = update(y_slot, coupling, (below_y, late_y), every, total)
    total = update(far_slot, coupling, (far_first,), UNITS_FIRST, total, whole=True)
    return last_update(far_slot, coupling, (far_first, *(far_last, on_a, on_b) * 4), total)


def solution(mesh):
    return jax.shard_map(
        on_device,
        mesh=mesh,
        in_specs=(P("gx", "gy", "gz"), P("gx", "gy", "gz"), P("gx", "gy", "gz")),
        out_specs=P("gx", "gy", "gz"),
        check_vma=False,
    )
```
